512 devices in a mesh: ea: 4 (over y), row: 16 (over z), col: 8 (over x, core).
Axes of the slice: x: 4, y: 4, z: 16, core: 2. Of those that a mesh axis runs over, the one named last changes fastest.
Arguments:
- weights: float32 [4, 1024, 2048], P('ea', 'row', 'col'), parts along dimension 0, may hold values from -6 to 6
- codebook: float32 [4, 16, 2, 256], P('ea', 'col'), parts along dimension 0, may hold values from -4 to 4
- assign: int32 [4, 1024, 1024], P('ea', 'row', 'col'), parts along dimension 0, may hold values from 0 to 255
- chol_upper: float32 [4, 2048, 2048], P('ea', 'row', 'col'), parts along dimension 0, may hold values from 0 to 1.4, as said below
- inv_blocks: float32 [4, 16, 128, 128], P('ea', 'col'), parts along dimension 0, may hold values from -1 to 1.5, as said below
Outputs:
- errors: float32 [4, 1024, 2048], P('ea', 'row', 'col'), parts along dimension 0
- row_loss: float32 [4, 1024], P('ea', 'row'), parts along dimension 0
- codeword_mass: float32 [4, 16, 256], P('ea', 'col'), parts along dimension 0
The draws below stay inside these ranges and needn't reach their ends.
There are 4 independent parts, one for each index of `ea`. The reference program is written for one: setup_inputs(seed, part) draws one part's arguments, and reference() takes and returns one part's arrays. A program takes and returns all parts, laid end to end along the dimension named above; each array names one. Nothing has to cross between parts.
Inputs may be any that keep to these rules, and one draw needn't show every extreme that they name: `chol_upper`: upper triangular with a positive diagonal. inv_blocks[x, b] is the inverse of the diagonal block of chol_upper[x] on rows and columns [b * 128, (b + 1) * 128).
All inputs are finite; a program needn't handle non-finite values.
Results may differ from the reference program's by a relative error of at most 0.0001.
Values sent between devices are 32-bit elements; how exact they have to be, the bound alone decides.
A program may use at most 64 MiB of HBM per device.

```python
import jax
import jax.numpy as jnp
from jax import lax

EXP_PART = 1
COLS = 2048
BLOCK = 128
CODES = 256
ROWS = 1024
NBLK = 16


def upper_factor(key):
    folded = jax.random.fold_in(key, 7)
    key_diag, key_near, key_far = jax.random.split(folded, 3)
    diagonal = jax.random.uniform(key_diag, (EXP_PART, COLS), jnp.float32, 0.7, 1.4)
    near_part = jax.random.uniform(key_near, (EXP_PART, COLS, COLS), jnp.float32, 0.0, 0.03)
    far_part = jax.random.uniform(key_far, (EXP_PART, COLS, COLS), jnp.float32, 0.0, 0.03)
    positions = jnp.arange(COLS, dtype=jnp.int32)
    same_block = positions[:, None] // BLOCK == positions[None, :] // BLOCK
    strictly_upper = positions[:, None] < positions[None, :]
    offdiag = jnp.where(same_block[None], near_part, far_part) * strictly_upper[None].astype(jnp.float32)
    return offdiag + diagonal[:, :, None] * jnp.eye(COLS, dtype=jnp.float32)[None]


def draw_chol_upper(key, part):
    return upper_factor(key)


def draw_inv_blocks(key, part):
    factor = upper_factor(key)
    blocked = factor.reshape(EXP_PART, NBLK, BLOCK, NBLK, BLOCK)
    which = jnp.arange(NBLK, dtype=jnp.int32)
    diagonal_blocks = jnp.transpose(blocked[:, which, :, which, :], (1, 0, 2, 3))
    return jnp.linalg.inv(diagonal_blocks)


def place_ends(array, key, smallest, high):
    shape = array.shape
    place = [jax.random.randint(jax.random.fold_in(key, axis), (), 0, shape[axis]) for axis in range(len(shape))]
    array = array.at[tuple(place)].set(smallest)
    longest = shape.index(max(shape))
    place[longest] = (place[longest] + 1) % shape[longest]
    return array.at[tuple(place)].set(high)


def levels(stream_key, shape, cuts, least, top_value):
    gain, own = 1.0, jax.random.fold_in(stream_key, 6)
    for axis_at, blocks in cuts:
        draws = jnp.exp(jax.random.uniform(jax.random.fold_in(own, axis_at), (blocks,), jnp.float32, least / len(cuts), top_value / len(cuts)))
        gain = gain * jnp.repeat(draws, shape[axis_at] // blocks).reshape([-1 if axis == axis_at else 1 for axis in range(len(shape))])
    return gain


def gaussian(key, dims, width, bound, shards=(), kind=jnp.bfloat16):
    drawn = width * jax.random.normal(key, dims, jnp.float32)
    if shards:
        drawn = drawn * levels(key, dims, shards, -0.22, 0.18)
    return jnp.clip(drawn, -bound, bound).astype(kind)


def setup_inputs(seed: int = 0, part: int = 0) -> dict:
    key_of = jax.random.split(jax.random.key(seed), 6)
    own_keys = jax.random.split(jax.random.fold_in(key_of[5], part), 6)
    weights = gaussian(own_keys[0], (EXP_PART, ROWS, COLS), 1.0, 6.0, ((1, 16), (2, 8)), jnp.float32)
    codebook = gaussian(own_keys[1], (EXP_PART, NBLK, 2, CODES), 1.0, 4.0, ((1, 8),), jnp.float32)
    assign = place_ends(jax.random.randint(own_keys[2], (EXP_PART, ROWS, COLS // 2), 0, CODES), jax.random.fold_in(own_keys[2], 1), 0, CODES - 1).astype(jnp.int32)
    chol_upper = draw_chol_upper(jax.random.fold_in(jax.random.fold_in(key_of[5], part), 71), part)
    inv_blocks = draw_inv_blocks(jax.random.fold_in(jax.random.fold_in(key_of[5], part), 71), part)
    return {"weights": weights, "codebook": codebook, "assign": assign, "chol_upper": chol_upper, "inv_blocks": inv_blocks}


def lookup(codebook, assign, half_block, code_count):
    pair_count = assign.shape[2]
    offsets = jnp.arange(pair_count, dtype=jnp.int32) // half_block * code_count
    flat_index = (assign + offsets[None, None, :]).astype(jnp.int32)
    experts = codebook.shape[0]
    code_table = jnp.transpose(codebook, (0, 2, 1, 3)).reshape(experts, 2, -1)

    def select(rows_table, indices):
        return jnp.stack([jnp.take(rows_table[0], indices), jnp.take(rows_table[1], indices)], axis=-1)
    picked = jax.vmap(select)(code_table, flat_index)
    return (picked.reshape(assign.shape[0], assign.shape[1], 2 * pair_count), flat_index)

def mass_by_code(errors, flat_index, segments):
    squared = errors * errors
    extent = errors.shape
    paired = squared.reshape(extent[0], extent[1], extent[2] // 2, 2).sum(axis=3)

    def summed(values, labels):
        return jax.ops.segment_sum(values.reshape(-1), labels.reshape(-1), num_segments=segments)
    return jax.vmap(summed)(paired, flat_index)

def reference(weights, codebook, assign, chol_upper, inv_blocks):
    quantized, flat_index = lookup(codebook, assign, BLOCK // 2, CODES)
    current = weights
    pieces = []
    for number in range(NBLK):
        first_col = number * BLOCK
        finish = first_col + BLOCK
        error_block = jnp.einsum('xrc,xcd->xrd', current[:, :, first_col:finish] - quantized[:, :, first_col:finish], inv_blocks[:, number], precision=lax.Precision.HIGHEST)
        pieces.append(error_block)
        if finish < COLS:
            change = jnp.einsum('xrc,xcd->xrd', error_block, chol_upper[:, first_col:finish, finish:], precision=lax.Precision.HIGHEST)
            current = jnp.concatenate([current[:, :, :finish], current[:, :, finish:] - change], axis=2)
    errors = jnp.concatenate(pieces, axis=2)
    row_loss = jnp.sum(errors * errors, axis=2)
    codeword_mass = mass_by_code(errors, flat_index, NBLK * CODES).reshape(EXP_PART, NBLK, CODES)
    return (errors, row_loss, codeword_mass)
```

```python
import functools

import jax
import jax.numpy as jnp
from jax import lax
from jax.experimental import pallas as pl
from jax.experimental.pallas import tpu as pltpu
from jax.sharding import PartitionSpec as P

MESH = pl.DeviceIdType.MESH
HI = lax.Precision.HIGHEST
F32 = jnp.float32
BF = jnp.bfloat16


def dot(a, b):
    return jnp.dot(a, b, precision=HI, preferred_element_type=F32)


def pieces(x):
    high = x.astype(BF)
    rest = x - high.astype(F32)
    mid = rest.astype(BF)
    low = (rest - mid.astype(F32)).astype(BF)
    return high, mid, low


def wide_codes(codes, block):
    rows = codes.shape[0]
    place = lax.broadcasted_iota(jnp.int32, (rows, 128), 1) // 2 + block * 64
    return jnp.take_along_axis(codes, place, axis=1)


def looked_up(table, wide):
    rows = wide.shape[0]
    low = jnp.bitwise_and(wide, 127)
    second = lax.broadcasted_iota(jnp.int32, (rows, 128), 1) % 2 == 1

    def from_half(k, half):
        row = table[k : k + 1, half * 128 : half * 128 + 128]
        return jnp.take_along_axis(jnp.broadcast_to(row, (rows, 128)), low, axis=1)

    def from_component(k):
        return jnp.where(wide >= 128, from_half(k, 1), from_half(k, 0))

    return jnp.where(second, from_component(1), from_component(0))


def mass_of(squared, wide):
    rows = squared.shape[0]
    upper = jnp.right_shift(wide, 4)
    lower = jnp.bitwise_and(wide, 15)
    level = lax.broadcasted_iota(jnp.int32, (16, 128), 0)
    left, right = [], []
    for r in range(rows):
        left.append(jnp.where(upper[r : r + 1, :] == level, squared[r : r + 1, :], 0.0))
        right.append(jnp.where(lower[r : r + 1, :] == level, 1.0, 0.0).astype(BF))
    spread = jnp.concatenate(pieces(jnp.concatenate(left, axis=1)), axis=0)
    hot = jnp.concatenate(right, axis=1)
    summed = lax.dot_general(spread, hot, (((1,), (1,)), ((), ())), preferred_element_type=F32)
    table = summed[0:16] + summed[16:32] + summed[32:48]
    lane = lax.broadcasted_iota(jnp.int32, (16, 128), 1)
    pick = jnp.where(lane % 16 == level, 1.0, 0.0)
    repeated = dot(table, pick)
    kept = jnp.where(lane // 16 == level % 8, repeated, 0.0)
    return jnp.concatenate(
        [jnp.sum(kept[0:8], axis=0, keepdims=True), jnp.sum(kept[8:16], axis=0, keepdims=True)],
        axis=0,
    )


def kernel(
    depth, cols,
    w_hbm, c_hbm, a_hbm, u_hbm, i_hbm,
    err_ref, loss_ref, mass_ref,
    wb, ab, cb, ib, u, xs, es, full_a, va, vh, vb, losses, masses,
    local_sem, pre_send, pre_recv, ring_send, ring_recv, side_send, side_recv,
    stage_send, stage_recv, back_send, back_recv, loss_send, loss_recv, mass_send, mass_recv, entered,
):
    z = lax.axis_index("row")
    c = lax.axis_index("col")
    h = lax.rem(c, 2)
    x = c // 2
    other = 1 - h
    partner = c + 1 - 2 * h
    chips = cols // 2
    rows = wb.shape[1]
    up = lax.rem(z + 1, depth)
    down = lax.rem(z + depth - 1, depth)
    far_up, far_down = depth // 2, (depth - 1) // 2

    mine = pl.ds(pl.multiple_of(h * rows, 8), rows)
    theirs = pl.ds(pl.multiple_of(other * rows, 8), rows)
    local = [
        pltpu.make_async_copy(u_hbm.at[0], u.at[h, z], local_sem.at[0]),
        pltpu.make_async_copy(i_hbm.at[0], ib.at[h], local_sem.at[1]),
        pltpu.make_async_copy(c_hbm.at[0], cb.at[h], local_sem.at[2]),
        pltpu.make_async_copy(w_hbm.at[0, mine], wb.at[h], local_sem.at[3]),
        pltpu.make_async_copy(a_hbm.at[0], full_a, local_sem.at[4]),
    ]
    for copy in local:
        copy.start()

    barrier = pltpu.get_barrier_semaphore()
    for to in (up, down):
        pl.semaphore_signal(barrier, inc=1, device_id={"row": to}, device_id_type=MESH)
    for d in range(1, cols):
        pl.semaphore_signal(
            barrier, inc=1, device_id={"col": lax.rem(c + d, cols)}, device_id_type=MESH
        )
    pl.semaphore_wait(barrier, cols + 1)

    def remote(src, dst, send, recv, **to):
        return pltpu.make_async_remote_copy(
            src_ref=src, dst_ref=dst, send_sem=send, recv_sem=recv, device_id=to,
            device_id_type=MESH,
        )

    def needed(b, column):
        return b <= 2 * column

    def ring_copy(b, way, step):
        return remote(
            u.at[h, b], u.at[h, b], ring_send.at[way, step], ring_recv.at[way, step],
            row=(up if way == 0 else down),
        )

    def side_copy(half, b):
        return remote(u.at[half, b], u.at[half, b], side_send.at[b], side_recv.at[b], col=partner)

    local[0].wait()

    @pl.when(needed(z, c))
    def _():
        ring_copy(z, 0, 1).start()
        ring_copy(z, 1, 1).start()
        side_copy(h, z).start()

    local[1].wait()
    local[2].wait()
    local[4].wait()
    pre = [
        remote(ib.at[h], ib.at[h], pre_send.at[0], pre_recv.at[0], col=partner),
        remote(cb.at[h], cb.at[h], pre_send.at[1], pre_recv.at[1], col=partner),
        remote(w_hbm.at[0, theirs], wb.at[h], pre_send.at[2], pre_recv.at[2], col=partner),
        remote(full_a.at[theirs], ab.at[h], pre_send.at[3], pre_recv.at[3], col=partner),
    ]
    for copy in pre:
        copy.start()
    local[3].wait()
    ab[h] = full_a[mine]

    def ring_step(step, carry):
        for way, farthest in ((0, far_up), (1, far_down)):
            b = lax.rem(z + (depth - step if way == 0 else step), depth)

            @pl.when(jnp.logical_and(step > 1, step <= farthest))
            def _():
                pl.semaphore_wait(entered.at[way], 1)

            @pl.when(step < farthest)
            def _():
                pl.semaphore_signal(
                    entered.at[way], inc=1, device_id={"row": up if way == 0 else down},
                    device_id_type=MESH,
                )

            @pl.when(jnp.logical_and(needed(b, c), step <= farthest))
            def _():
                ring_copy(b, way, step).wait_recv()

                @pl.when(step < farthest)
                def _():
                    ring_copy(b, way, step + 1).start()

                side_copy(h, b).start()

        return carry

    lax.fori_loop(1, far_up + 1, ring_step, 0)

    for copy in pre:
        copy.wait_recv()

    for g in range(2):
        for block in range(2):
            wide = wide_codes(ab[g], block)
            part = slice(block * 128, block * 128 + 128)
            xs[g, :, part] = wb[g, :, part] - looked_up(cb[g, block], wide)

    def side_wait(b, carry):
        @pl.when(needed(b, partner))
        def _():
            side_copy(other, b).wait_recv()

        return carry

    lax.fori_loop(0, depth, side_wait, 0)

    base = 4 * x
    zero = jnp.zeros((128, 128), F32)
    for g, out in ((0, va), (1, vb)):
        first, second = ib[g, 0], ib[g, 1]
        between = u[g, base + 2 * g][:, 128:256]
        corner = -dot(first, dot(between, second))
        out[0:128, 0:128] = first
        out[0:128, 128:256] = corner
        out[128:256, 0:128] = zero
        out[128:256, 128:256] = second
    vh[...] = -dot(va[...], dot(u[1, pl.ds(base, 2)].reshape(256, 256), vb[...]))

    def stage_copy(s, d):
        return remote(
            es.at[s], es.at[s], stage_send.at[d], stage_recv.at[s], col=lax.rem(c + 2 * d, cols)
        )

    def absorb(s, carry):
        stage_copy(s, 1).wait_recv()
        for g in range(2):
            panel = u[g, pl.ds(4 * s, 4)].reshape(512, 256)
            both = jnp.concatenate([es[s, 0], es[s, 1]], axis=1)
            xs[g] = xs[g] - dot(both, panel)
        return carry

    lax.fori_loop(0, x, absorb, 0)
    e0 = dot(xs[0], va[...])
    e1 = dot(xs[0], vh[...]) + dot(xs[1], vb[...])
    es[x, 0] = e0
    es[x, 1] = e1
    for d in range(1, chips):

        @pl.when(x + d < chips)
        def _(d=d):
            stage_copy(x, d).start()

    back = remote(es.at[x, other], err_ref.at[0, mine], back_send, back_recv, col=partner)
    back.start()
    err_ref[0, mine, :] = es[x, h]
    back.wait_recv()

    squared = err_ref[0] * err_ref[0]
    sums = lax.dot_general(
        jnp.ones((8, 256), F32), squared, (((1,), (1,)), ((), ())), precision=HI,
        preferred_element_type=F32,
    )
    losses[c] = sums

    def loss_copy(d):
        return remote(
            losses.at[c], losses.at[c], loss_send.at[d], loss_recv.at[c],
            col=lax.rem(c + d, cols),
        )

    for d in range(1, cols):
        loss_copy(d).start()

    for block in range(2):
        wide = wide_codes(full_a[...], block)
        found = mass_of(squared[:, block * 128 : block * 128 + 128], wide)
        masses[z, 2 * block : 2 * block + 2, :] = found

    def mass_copy(d):
        return remote(
            masses.at[z], masses.at[z], mass_send.at[d], mass_recv.at[z],
            row=lax.rem(z + d, depth),
        )

    def mass_start(d, carry):
        mass_copy(d).start()
        return carry

    lax.fori_loop(1, depth, mass_start, 0)

    def loss_wait(d, carry):
        source = lax.rem(c + d, cols)
        remote(
            losses.at[source], losses.at[source], loss_send.at[d], loss_recv.at[source], col=source
        ).wait_recv()
        return carry

    lax.fori_loop(1, cols, loss_wait, 0)
    loss_ref[...] = jnp.sum(losses[...], axis=0)[0:1, :]

    def mass_wait(d, carry):
        source = lax.rem(z + d, depth)
        remote(
            masses.at[source], masses.at[source], mass_send.at[d], mass_recv.at[source], row=source
        ).wait_recv()
        return carry

    lax.fori_loop(1, depth, mass_wait, 0)
    total = jnp.sum(masses[...], axis=0)
    for block in range(2):
        for part in range(2):
            at = 2 * block + part
            mass_ref[0, block : block + 1, part * 128 : part * 128 + 128] = total[at : at + 1, :]

    @pl.when(needed(z, c))
    def _():
        ring_copy(z, 0, 1).wait_send()
        ring_copy(z, 1, 1).wait_send()
        side_copy(h, z).wait_send()

    def ring_drain(step, carry):
        for way, farthest in ((0, far_up), (1, far_down)):
            b = lax.rem(z + (depth - step if way == 0 else step), depth)

            @pl.when(jnp.logical_and(needed(b, c), step <= farthest))
            def _():
                @pl.when(step < farthest)
                def _():
                    ring_copy(b, way, step + 1).wait_send()

                side_copy(h, b).wait_send()

        return carry

    lax.fori_loop(1, far_up + 1, ring_drain, 0)
    for copy in pre:
        copy.wait_send()
    for d in range(1, chips):

        @pl.when(x + d < chips)
        def _(d=d):
            stage_copy(x, d).wait_send()

    back.wait_send()
    for d in range(1, cols):
        loss_copy(d).wait_send()

    def mass_drain(d, carry):
        mass_copy(d).wait_send()
        return carry

    lax.fori_loop(1, depth, mass_drain, 0)


def local(weights, codebook, assign, chol_upper, inv_blocks):
    depth, cols = lax.axis_size("row"), lax.axis_size("col")
    rows = weights.shape[1] // 2
    hbm = pl.BlockSpec(memory_space=pl.ANY)
    vmem = pl.BlockSpec(memory_space=pltpu.VMEM)
    dma = pltpu.SemaphoreType.DMA
    return tuple(
        pl.pallas_call(
            functools.partial(kernel, depth, cols),
            out_shape=(
                jax.ShapeDtypeStruct(weights.shape, F32),
                jax.ShapeDtypeStruct((1, 2 * rows), F32),
                jax.ShapeDtypeStruct((1, 2, 256), F32),
            ),
            in_specs=[hbm] * 5,
            out_specs=(vmem, vmem, vmem),
            scratch_shapes=[
                pltpu.VMEM((2, rows, 256), F32),
                pltpu.VMEM((2, rows, 128), jnp.int32),
                pltpu.VMEM((2, 2, 2, 256), F32),
                pltpu.VMEM((2, 2, 128, 128), F32),
                pltpu.VMEM((2, depth, 128, 256), F32),
                pltpu.VMEM((2, rows, 256), F32),
                pltpu.VMEM((cols // 2, 2, rows, 256), F32),
                pltpu.VMEM((2 * rows, 128), jnp.int32),
                pltpu.VMEM((256, 256), F32),
                pltpu.VMEM((256, 256), F32),
                pltpu.VMEM((256, 256), F32),
                pltpu.VMEM((cols, 8, 2 * rows), F32),
                pltpu.VMEM((depth, 4, 128), F32),
                dma((5,)),
                dma((4,)),
                dma((4,)),
                dma((2, depth // 2 + 1)),
                dma((2, depth // 2 + 1)),
                dma((depth,)),
                dma((depth,)),
                dma((cols // 2,)),
                dma((cols // 2,)),
                dma,
                dma,
                dma((cols,)),
                dma((cols,)),
                dma((depth,)),
                dma((depth,)),
                pltpu.SemaphoreType.REGULAR((2,)),
            ],
            compiler_params=pltpu.CompilerParams(
                collective_id=0, has_side_effects=True, vmem_limit_bytes=48 * 1024 * 1024
            ),
        )(weights, codebook, assign, chol_upper, inv_blocks)
    )


def solution(mesh):
    return jax.shard_map(
        local,
        mesh=mesh,
        in_specs=(
            P("ea", "row", "col"),
            P("ea", "col", None, None),
            P("ea", "row", "col"),
            P("ea", "row", "col"),
            P("ea", "col", None, None),
        ),
        out_specs=(P("ea", "row", "col"), P("ea", "row"), P("ea", "col", None)),
        check_vma=False,
    )
```
